128 devices in a mesh: expert: 8 (over x, core), tile: 16 (over z, y).
Axes of the slice: x: 4, y: 4, z: 4, core: 2. Of those that a mesh axis runs over, the one named last changes fastest.
Arguments:
- weight: bfloat16 [8, 2048, 8192], P('expert', None, 'tile'), may hold values from -6 to 6
- grad: bfloat16 [8, 2048, 8192], P('expert', None, 'tile'), may hold values from -24 to 24, as said below
- first_moment: float32 [8, 2048, 8192], P('expert', None, 'tile'), may hold values from -6 to 6
- second_moment: float32 [8, 2048, 8192], P('expert', None, 'tile'), may hold values from 0.25 to 4
- left_basis: bfloat16 [8, 1024, 2048], P('expert', None, 'tile'), may hold values from -1 to 1, as said below
- right_basis: bfloat16 [8, 1024, 8192], P('expert', None, 'tile'), may hold values from -1 to 1, as said below
Outputs:
- new_weight: bfloat16 [8, 2048, 8192], P('expert', None, 'tile')
- new_first: float32 [8, 2048, 8192], P('expert', None, 'tile')
- new_second: float32 [8, 2048, 8192], P('expert', None, 'tile')
The draws below stay inside these ranges and needn't reach their ends.
Inputs may be any that keep to these rules, and one draw needn't show every extreme that they name: `grad`: scaled values. `left_basis`: every diagonal block is orthogonal before rounding to bfloat16. `right_basis`: every diagonal block is orthogonal before rounding to bfloat16.
All inputs are finite; a program needn't handle non-finite values.
Results may differ from the reference program's by a relative error of at most 0.0045.
Values may be sent and summed in bfloat16 or wider, within the bound.
No kernel may reach another device: no remote copies, remote signals or barrier semaphores. Data moves between devices by JAX's collectives and lax.ppermute only.
A program may use at most 128 MiB of HBM per device.

```python
import math
import jax
import jax.numpy as jnp
from jax import lax

D = 2048
FF = 8192
BLOCK = 1024
EXPERTS = 8


def draw_grad(key, part):
    first_key, second_key = jax.random.split(jax.random.fold_in(key, 11), 2)
    noise = jnp.clip(jax.random.normal(first_key, (EXPERTS, D, FF), jnp.float32), -6.0, 6.0)
    logs = jax.random.uniform(second_key, (EXPERTS, 1, FF // 128), jnp.float32, math.log(0.5), math.log(4.0))
    scales = jnp.repeat(jnp.exp(logs), 128, axis=2)
    return (noise * scales).astype(jnp.bfloat16)


def orthogonal_blocks(key, count):
    normal = jax.random.normal(key, (EXPERTS, count, BLOCK, BLOCK), jnp.float32)
    factor, upper = jnp.linalg.qr(normal)
    return jnp.transpose(factor, (0, 2, 1, 3)).reshape(EXPERTS, BLOCK, count * BLOCK)


def draw_left_basis(key, part):
    return orthogonal_blocks(jax.random.fold_in(key, 23), D // BLOCK).astype(jnp.bfloat16)


def draw_right_basis(key, part):
    return orthogonal_blocks(jax.random.fold_in(key, 37), FF // BLOCK).astype(jnp.bfloat16)


def shard_levels(rng, shape, cuts, smallest, high):
    loudness, own = 1.0, jax.random.fold_in(rng, 6)
    for dim, shards_of in cuts:
        steps = jnp.exp(jax.random.uniform(jax.random.fold_in(own, dim), (shards_of,), jnp.float32, smallest / len(cuts), high / len(cuts)))
        loudness = loudness * jnp.repeat(steps, shape[dim] // shards_of).reshape([-1 if axis == dim else 1 for axis in range(len(shape))])
    return loudness


def normal_values(stream_key, shape, scale, bound, cuts=(), held_as=jnp.bfloat16):
    entries = jax.random.normal(stream_key, shape, jnp.float32) * scale
    if len(cuts) > 0:
        entries = shard_levels(stream_key, shape, cuts, -0.22, 0.18) * entries
    return jnp.clip(entries, min=-bound, max=bound).astype(held_as)


def setup_inputs(seed: int = 0) -> dict:
    keys = jax.random.split(jax.random.key(seed), 7)
    return {
        "weight": normal_values(keys[0], (EXPERTS, D, FF), 1.0, 6.0, ((0, 8), (2, 16))),
        "grad": draw_grad(jax.random.fold_in(keys[6], 71), 0),
        "first_moment": normal_values(keys[2], (EXPERTS, D, FF), 1.0, 6.0, ((0, 8), (2, 16)), jnp.float32),
        "second_moment": jnp.clip(jnp.exp(math.log(4.0) - 2.7725887 * jax.random.uniform(keys[3], (EXPERTS, D, FF), jnp.float32) ** shard_levels(keys[3], (EXPERTS, D, FF), ((0, 8), (2, 16)), -0.2, 0.2)), 0.25, 4.0),
        "left_basis": draw_left_basis(jax.random.fold_in(keys[6], 71), 0),
        "right_basis": draw_right_basis(jax.random.fold_in(keys[6], 71), 0),
    }


beta_one = 0.9
beta_two = 0.95
epsilon = 1e-08
learn_rate = 0.25
decay_rate = 0.1

def reference(weight, grad, first_moment, second_moment, left_basis, right_basis):
    total = jnp.sum(jnp.square(grad.astype(jnp.float32)))
    count = EXPERTS * D * FF
    clip = 1.0 / jnp.maximum(1.0, jnp.sqrt(total / count))
    left_count = D // BLOCK
    right_count = FF // BLOCK
    highest = lax.Precision.HIGHEST

    def one_expert(items):
        old_weight, gradient, moment_one, moment_two, left_one, right_one = items
        left4 = left_one.astype(jnp.float32).reshape(BLOCK, left_count, BLOCK)
        right4 = right_one.astype(jnp.float32).reshape(BLOCK, right_count, BLOCK)
        grad4 = gradient.astype(jnp.float32).reshape(left_count, BLOCK, FF)
        rotated_left = jnp.einsum('kbi,bkf->bif', left4, grad4, precision=highest).reshape(D, FF).astype(jnp.bfloat16)
        rows_right = rotated_left.astype(jnp.float32).reshape(D, right_count, BLOCK)
        rotated = jnp.einsum('dck,kcj->dcj', rows_right, right4, precision=highest).reshape(D, FF)
        clipped = clip * rotated
        new_first = beta_one * moment_one + (1.0 - beta_one) * clipped
        new_second = beta_two * moment_two + (1.0 - beta_two) * clipped * clipped
        update = (new_first / (jnp.sqrt(new_second) + epsilon)).astype(jnp.bfloat16)
        update4 = update.astype(jnp.float32).reshape(D, right_count, BLOCK)
        back_right = jnp.einsum('dcj,kcj->dck', update4, right4, precision=highest).reshape(D, FF).astype(jnp.bfloat16)
        back4 = back_right.astype(jnp.float32).reshape(left_count, BLOCK, FF)
        back = jnp.einsum('kbi,bif->bkf', left4, back4, precision=highest).reshape(D, FF)
        weight32 = old_weight.astype(jnp.float32)
        new_weight = (weight32 - learn_rate * (back + decay_rate * weight32)).astype(jnp.bfloat16)
        return (new_weight, new_first, new_second)
    new_weight, new_first, new_second = lax.map(one_expert, (weight, grad, first_moment, second_moment, left_basis, right_basis))
    return (new_weight, new_first, new_second)
```

```python
import functools

import jax
import jax.numpy as jnp
from jax import lax
from jax.experimental import pallas as pl
from jax.experimental.pallas import tpu as pltpu
from jax.sharding import Mesh
from jax.sharding import PartitionSpec as P

AXES = ("x", "core", "z", "y")
EXPERT = ("x", "core")
TILE = ("z", "y")

beta_one = 0.9
beta_two = 0.95
epsilon = 1e-08
learn_rate = 0.25
decay_rate = 0.1


f32 = jnp.float32
bf16 = jnp.bfloat16
ANY = pl.BlockSpec(memory_space=pl.ANY)


def cost(flops, bytes_accessed):
    return pl.CostEstimate(flops=flops, bytes_accessed=bytes_accessed, transcendentals=0)


def permute(value, axis, target):
    pairs = [(source, target(source)) for source in range(lax.axis_size(axis))]
    return lax.ppermute(value, axis, pairs)


def pair(y):
    return y ^ 1


def side(y):
    return 3 - y


def after(z):
    return (z + 1) % 4


def before(z):
    return (z + 3) % 4


def opposite(z):
    return (z + 2) % 4


def whole_sum(value):
    value = value + permute(value, "y", pair)
    for _ in range(1):
        value = value + permute(value, "core", pair)
    value = sum(
        [permute(value, "x", f) for f in (after, before, opposite)],
        value,
    )
    value = value + permute(value, "y", side)
    value = sum(
        [permute(value, "z", f) for f in (after, before, opposite)],
        value,
    )
    return value


def gather_left(shard):
    c0 = shard
    c1 = permute(c0, "y", pair)
    c2 = permute(c0, "y", side)
    c3 = permute(c1, "y", side)
    columns = (c0, c1, c2, c3)
    ups = [permute(c, "z", after) for c in columns]
    downs = [permute(c, "z", before) for c in columns]
    relays = [permute(ups[i], "z", after) for i in (0, 1)]
    relays += [permute(downs[i], "z", before) for i in (2, 3)]
    return [*columns, *ups, *downs, *relays]


def forward_kernel(block_index, chained, *refs):
    clip_ref = refs[0]
    shards = refs[1:17]
    own_ref, other_ref, right_ref, first_ref, second_ref = refs[17:22]
    rest = refs[24:] if chained else refs[22:]
    new_first_ref, new_second_ref, left_ref, send_ref, keep_ref, sems = rest
    width = right_ref.shape[2]
    rows = new_first_ref.shape[1]
    z = lax.axis_index("z")
    y = lax.axis_index("y")
    step = pl.program_id(0)
    partner = lax.rem(y + 1, 2) * 2 - 1 + y

    @pl.when(step == 0)
    def _():
        columns = (y, partner, 3 - y, 3 - partner)
        for phase in range(2):
            for group, distance in enumerate((0, 3, 1, 2)):
                row = lax.rem(z + distance, 4)

                @pl.when(lax.div(row, 2) == block_index)
                def _():
                    for k in range(4):
                        slot = lax.rem(row, 2) * 4 + columns[k]
                        lanes = pl.ds(pl.multiple_of(slot * 128, 128), 128)
                        copy = pltpu.make_async_copy(
                            shards[group * 4 + k].at[0],
                            left_ref.at[:, lanes],
                            sems.at[group * 4 + k],
                        )
                        if phase == 0:
                            copy.start()
                        else:
                            copy.wait()

    position = lax.rem(y, 2)
    lanes = pl.ds(pl.multiple_of(step * rows, rows), rows)
    left = left_ref[:, lanes]
    right_own = right_ref[0, pl.ds(pl.multiple_of(position * width, width), width), :]
    right_other = right_ref[0, pl.ds(pl.multiple_of((1 - position) * width, width), width), :]
    tn = (((0,), (0,)), ((), ()))
    nt = (((1,), (1,)), ((), ()))
    rotated_own = lax.dot_general(left, own_ref[0], tn, preferred_element_type=f32).astype(bf16)
    rotated_other = lax.dot_general(left, other_ref[0], tn, preferred_element_type=f32).astype(bf16)
    rotated = jnp.dot(rotated_own, right_own, preferred_element_type=f32) + jnp.dot(
        rotated_other, right_other, preferred_element_type=f32
    )
    clipped = clip_ref[0, 0] * rotated
    new_first = beta_one * first_ref[0] + (1.0 - beta_one) * clipped
    new_second = beta_two * second_ref[0] + (1.0 - beta_two) * clipped * clipped
    new_first_ref[0] = new_first
    new_second_ref[0] = new_second
    update = (new_first / (jnp.sqrt(new_second) + epsilon)).astype(bf16)
    send_ref[...] = lax.dot_general(update, right_other, nt, preferred_element_type=f32).astype(bf16)
    keep_ref[...] = lax.dot_general(update, right_own, nt, preferred_element_type=f32).astype(bf16)


def forward(block_index, clip, shards, grad, other, right, first, second, previous):
    _, all_rows, width = grad.shape
    block = right.shape[1]
    rows = 256
    steps = block // rows
    chained = previous is not None
    moment = pl.BlockSpec((1, rows, width), lambda s: (0, block_index * steps + s, 0))
    term = pl.BlockSpec((rows, width), lambda s: (s, 0))
    moments = jax.ShapeDtypeStruct((1, all_rows, width), f32)
    terms = jax.ShapeDtypeStruct((block, width), bf16)
    in_specs = [pl.BlockSpec(memory_space=pltpu.SMEM)] + [ANY] * 16
    in_specs += [
        pl.BlockSpec((1, block, width), lambda s: (0, block_index, 0)),
        pl.BlockSpec((1, block, width), lambda s: (0, 0, 0)),
        pl.BlockSpec((1, block, width), lambda s: (0, 0, 0)),
        moment,
        moment,
    ]
    operands = [clip, *shards, grad, other, right, first, second]
    aliases = {}
    if chained:
        in_specs += [ANY, ANY]
        operands += list(previous)
        aliases = {22: 0, 23: 1}
    return pl.pallas_call(
        functools.partial(forward_kernel, block_index, chained),
        grid=(steps,),
        out_shape=[moments, moments, jax.ShapeDtypeStruct((block, block), bf16), terms, terms],
        in_specs=in_specs,
        out_specs=[moment, moment, pl.BlockSpec((block, block), lambda s: (0, 0)), term, term],
        scratch_shapes=[pltpu.SemaphoreType.DMA((16,))],
        input_output_aliases=aliases,
        cost_estimate=cost(8 * block * block * width, 16 * block * block),
        compiler_params=pltpu.CompilerParams(vmem_limit_bytes=48 * 1024 * 1024),
    )(*operands)


def back_kernel(left_ref, term_ref, out_ref):
    out_ref[...] = jnp.dot(left_ref[...], term_ref[...], preferred_element_type=f32).astype(bf16)


def back_send(left, term, start, count):
    block, width = term.shape
    rows = 256
    return pl.pallas_call(
        back_kernel,
        grid=(count // rows,),
        out_shape=jax.ShapeDtypeStruct((count, width), bf16),
        in_specs=[
            pl.BlockSpec((rows, block), lambda s: (start // rows + s, 0)),
            pl.BlockSpec((block, width), lambda s: (0, 0)),
        ],
        out_specs=pl.BlockSpec((rows, width), lambda s: (s, 0)),
        cost_estimate=cost(2 * count * block * width, 2 * count * block + 2 * block * width),
    )(left, term)


def base_kernel(left_ref, term_ref, weight_ref, out_ref):
    back = jnp.dot(left_ref[...], term_ref[...], preferred_element_type=f32)
    weight = weight_ref[0].astype(f32)
    out_ref[...] = weight - learn_rate * (back + decay_rate * weight)


def base(block_index, left, term, weight):
    block, width = term.shape
    rows = 256
    steps = block // rows
    return pl.pallas_call(
        base_kernel,
        grid=(steps,),
        out_shape=jax.ShapeDtypeStruct((block, width), f32),
        in_specs=[
            pl.BlockSpec((rows, block), lambda s: (s, 0)),
            pl.BlockSpec((block, width), lambda s: (0, 0)),
            pl.BlockSpec((1, rows, width), lambda s: (0, block_index * steps + s, 0)),
        ],
        out_specs=pl.BlockSpec((rows, width), lambda s: (s, 0)),
        cost_estimate=cost(2 * block * block * width, 8 * block * width),
    )(left, term, weight)


def finish_kernel(base_ref, received_ref, *refs):
    out_ref = refs[-1]
    out_ref[0] = (base_ref[...] - learn_rate * received_ref[...].astype(f32)).astype(bf16)


def finish(base_term, received, start, offset, total_rows, previous):
    count, width = received.shape
    rows = 128
    in_specs = [
        pl.BlockSpec((rows, width), lambda s: (offset // rows + s, 0)),
        pl.BlockSpec((rows, width), lambda s: (s, 0)),
    ]
    operands = [base_term, received]
    aliases = {}
    if previous is not None:
        in_specs.append(ANY)
        operands.append(previous)
        aliases = {2: 0}
    return pl.pallas_call(
        finish_kernel,
        grid=(count // rows,),
        out_shape=jax.ShapeDtypeStruct((1, total_rows, width), bf16),
        in_specs=in_specs,
        out_specs=pl.BlockSpec((1, rows, width), lambda s: (0, start // rows + s, 0)),
        input_output_aliases=aliases,
        cost_estimate=cost(2 * count * width, 8 * count * width),
    )(*operands)


def on_device(weight, grad, first_moment, second_moment, left_basis, right_basis):
    _, rows, width = grad.shape
    block = right_basis.shape[1]
    count = 8 * rows * width * 16

    other0 = permute(grad[:, :block], "y", pair)
    other1 = permute(grad[:, block:], "y", pair)
    local_total = jnp.sum(jnp.square(grad.astype(f32))).reshape(1, 1)
    total = whole_sum(local_total)
    clip = 1.0 / jnp.maximum(1.0, jnp.sqrt(total / count))
    shards = gather_left(left_basis)

    nf, ns, left0, send0, keep0 = forward(
        0, clip, shards, grad, other0, right_basis, first_moment, second_moment, None
    )
    back0 = back_send(left0, send0, 0, block)
    received0 = permute(back0, "y", pair)
    base0 = base(0, left0, keep0, weight)

    nf, ns, left1, send1, keep1 = forward(
        1, clip, shards, grad, other1, right_basis, first_moment, second_moment, (nf, ns)
    )
    pieces = ((0, 512), (512, 256), (768, 256))
    received1 = []
    for start, size in pieces:
        part = back_send(left1, send1, start, size)
        received1.append(permute(part, "y", pair))
    base1 = base(1, left1, keep1, weight)

    new_weight = finish(base0, received0, 0, 0, rows, None)
    for i, (start, size) in enumerate(pieces):
        new_weight = finish(base1, received1[i], block + start, start, rows, new_weight)
    return (new_weight, nf, ns)


def solution(mesh):
    finer = Mesh(mesh.devices.reshape(4, 2, 4, 4), AXES)
    spec = P(EXPERT, None, TILE)
    return jax.shard_map(
        on_device, mesh=finer, in_specs=(spec,) * 6, out_specs=(spec,) * 3, check_vma=False
    )
```

```python
import functools

import jax
import jax.numpy as jnp
from jax import lax
from jax.experimental import pallas as pl
from jax.experimental.pallas import tpu as pltpu
from jax.sharding import Mesh
from jax.sharding import PartitionSpec as P


AXES = ("x", "core", "z", "y")
EXPERT = ("x", "core")
TILE = ("z", "y")

beta_one = 0.9
beta_two = 0.95
epsilon = 1e-08
learn_rate = 0.25
decay_rate = 0.1


f32 = jnp.float32
bf16 = jnp.bfloat16
ANY = pl.BlockSpec(memory_space=pl.ANY)
MIB = 1024 * 1024
PIECES = ((0, 512), (512, 384), (896, 128))


def cost(flops, bytes_accessed):
    return pl.CostEstimate(flops=flops, bytes_accessed=bytes_accessed, transcendentals=0)


def limit(mib):
    return pltpu.CompilerParams(vmem_limit_bytes=mib * MIB)


def near(i):
    return i ^ 1


def far(i):
    return 3 - i


def permute(value, axis, target):
    pairs = [(source, target(source)) for source in range(lax.axis_size(axis))]
    return lax.ppermute(value, axis, pairs)


def every_sum(value):
    devices = lax.axis_size(AXES)
    return lax.all_to_all(jnp.broadcast_to(value, (devices, 1, 128)), AXES, 0, 0, tiled=True)


def gather_left(shard):
    row = jnp.concatenate((shard, permute(shard, "y", near)), axis=1)
    row_far = permute(row, "y", far)
    near0 = permute(row, "z", near)
    far0 = permute(row, "z", far)
    near1 = permute(row_far, "z", near)
    far1 = permute(row_far, "z", far)
    far2 = permute(jnp.concatenate((near0, near1), axis=1), "z", far)
    return row, (row, row_far, near0, near1), (far0, far1, far2)


def rotate_right_kernel(own_ref, other_ref, right_ref, out_ref):
    width = right_ref.shape[2]
    position = lax.rem(lax.axis_index("y"), 2)
    right_own = right_ref[0, pl.ds(pl.multiple_of(position * width, width), width), :]
    right_other = right_ref[0, pl.ds(pl.multiple_of((1 - position) * width, width), width), :]
    out_ref[...] = (
        jnp.dot(own_ref[0], right_own, preferred_element_type=f32)
        + jnp.dot(other_ref[0], right_other, preferred_element_type=f32)
    ).astype(bf16)


def rotate_right(own, other, right):
    _, block, width = own.shape
    rows = 256
    chunk = pl.BlockSpec((1, rows, width), lambda s: (0, s, 0))
    return pl.pallas_call(
        rotate_right_kernel,
        grid=(block // rows,),
        out_shape=jax.ShapeDtypeStruct((block, width), bf16),
        in_specs=[chunk, chunk, pl.BlockSpec((1, block, width), lambda s: (0, 0, 0))],
        out_specs=pl.BlockSpec((rows, width), lambda s: (s, 0)),
        cost_estimate=cost(4 * block * width * width, 8 * block * width),
        compiler_params=limit(58),
    )(own, other, right)


def moments_kernel(is_near, groups, count, block_ref, sums_ref, *refs):
    shards = refs[:groups]
    term_ref, right_ref, first_ref, second_ref = refs[groups : groups + 4]
    new_first_ref, new_second_ref, send_ref, turned_ref, left_ref, update_ref, sems = refs[-7:]
    width = right_ref.shape[2]
    block = left_ref.shape[0]
    rows = new_first_ref.shape[1]
    steps = block // rows
    z = lax.axis_index("z")
    y = lax.axis_index("y")
    step = pl.program_id(0)

    @pl.when(step == 0)
    def _():
        partner = y + 1 - 2 * lax.rem(y, 2)
        columns = (y, partner, 3 - y, 3 - partner)
        if is_near:
            parity = lax.rem(z, 2)
            places = [(0, 0, 0), (0, 1, 0), (1, 0, 0), (1, 1, 0), (2, 0, 1), (2, 1, 1), (3, 0, 1), (3, 1, 1)]
        else:
            parity = lax.rem(z + 1, 2)
            places = [(0, 0, 0), (0, 1, 0), (1, 0, 0), (1, 1, 0), (2, 0, 1), (2, 1, 1), (2, 2, 1), (2, 3, 1)]
        copies = []
        for k, (group, part, other_row) in enumerate(places):
            row = 1 - parity if other_row else parity
            slot = row * 4 + columns[k % 4]
            copies.append(
                pltpu.make_async_copy(
                    shards[group].at[0, pl.ds(part * block, block), :],
                    left_ref.at[:, pl.ds(pl.multiple_of(slot * 128, 128), 128)],
                    sems.at[k],
                )
            )
        for copy in copies:
            copy.start()
        for copy in copies:
            copy.wait()

    @pl.when(step < steps)
    def _():
        chunk = pl.ds(pl.multiple_of(step * rows, rows), rows)
        rotated = lax.dot_general(
            left_ref[:, chunk], term_ref[...], (((0,), (0,)), ((), ())), preferred_element_type=f32
        )
        total = jnp.sum(sums_ref[...], axis=0)
        clip = 1.0 / jnp.maximum(1.0, jnp.sqrt(total / count))
        clipped = jnp.concatenate([clip] * (width // 128), axis=1) * rotated
        new_first = beta_one * first_ref[0] + (1.0 - beta_one) * clipped
        new_second = beta_two * second_ref[0] + (1.0 - beta_two) * clipped * clipped
        new_first_ref[0] = new_first
        new_second_ref[0] = new_second
        update_ref[chunk, :] = (new_first / (jnp.sqrt(new_second) + epsilon)).astype(bf16)

    @pl.when(step >= steps)
    def _():
        position = lax.rem(y, 2)
        right_other = right_ref[0, pl.ds(pl.multiple_of((1 - position) * width, width), width), :]
        chunk = pl.ds(pl.multiple_of((step - steps) * rows, rows), rows)
        turned = jnp.dot(left_ref[chunk, :], update_ref[...], preferred_element_type=f32).astype(bf16)
        turned_ref[...] = turned
        send_ref[...] = lax.dot_general(
            turned, right_other, (((1,), (1,)), ((), ())), preferred_element_type=f32
        ).astype(bf16)


def moments(is_near, which, sums, shards, term, right, first, second, previous):
    _, all_rows, width = first.shape
    block = right.shape[1]
    rows = 256
    steps = block // rows
    groups = len(shards)
    count = sums.shape[0] * all_rows * width
    moment = pl.BlockSpec(
        (1, rows, width), lambda s, b: (0, b[0] * steps + jnp.minimum(s, steps - 1), 0)
    )
    late = pl.BlockSpec((rows, width), lambda s, b: (jnp.maximum(s - steps, 0), 0))
    whole = jax.ShapeDtypeStruct((1, all_rows, width), f32)
    part = jax.ShapeDtypeStruct((block, width), bf16)
    in_specs = [pl.BlockSpec(sums.shape, lambda s, b: (0, 0, 0))] + [ANY] * groups
    in_specs += [
        pl.BlockSpec((block, width), lambda s, b: (0, 0)),
        pl.BlockSpec((1, block, width), lambda s, b: (0, 0, 0)),
        moment,
        moment,
    ]
    operands = [which, sums, *shards, term, right, first, second]
    aliases = {}
    if previous is not None:
        in_specs += [ANY, ANY]
        aliases = {len(operands): 0, len(operands) + 1: 1}
        operands += list(previous)
    return pl.pallas_call(
        functools.partial(moments_kernel, is_near, groups, count),
        grid_spec=pltpu.PrefetchScalarGridSpec(
            num_scalar_prefetch=1,
            grid=(2 * steps,),
            in_specs=in_specs,
            out_specs=[moment, moment, late, late],
            scratch_shapes=[
                pltpu.VMEM((block, block), bf16),
                pltpu.VMEM((block, width), bf16),
                pltpu.SemaphoreType.DMA((8,)),
            ],
        ),
        out_shape=[whole, whole, part, part],
        input_output_aliases=aliases,
        cost_estimate=cost(5 * block * block * width, 20 * block * width),
        compiler_params=limit(58),
    )(*operands)


def base_kernel(block_ref, turned_ref, right_ref, weight_ref, out_ref):
    width = right_ref.shape[2]
    position = lax.rem(lax.axis_index("y"), 2)
    right_own = right_ref[0, pl.ds(pl.multiple_of(position * width, width), width), :]
    back = lax.dot_general(
        turned_ref[...], right_own, (((1,), (1,)), ((), ())), preferred_element_type=f32
    )
    weight = weight_ref[0].astype(f32)
    out_ref[...] = weight - learn_rate * (back + decay_rate * weight)


def base(which, turned, right, weight):
    block, width = turned.shape
    rows = 256
    steps = block // rows
    return pl.pallas_call(
        base_kernel,
        grid_spec=pltpu.PrefetchScalarGridSpec(
            num_scalar_prefetch=1,
            grid=(steps,),
            in_specs=[
                pl.BlockSpec((rows, width), lambda s, b: (s, 0)),
                pl.BlockSpec((1, block, width), lambda s, b: (0, 0, 0)),
                pl.BlockSpec((1, rows, width), lambda s, b: (0, b[0] * steps + s, 0)),
            ],
            out_specs=pl.BlockSpec((rows, width), lambda s, b: (s, 0)),
        ),
        out_shape=jax.ShapeDtypeStruct((block, width), f32),
        cost_estimate=cost(2 * block * width * width, 10 * block * width),
        compiler_params=limit(12),
    )(which, turned, right, weight)


def finish_kernel(block_ref, base_ref, received_ref, *refs):
    refs[-1][0] = (base_ref[...] - learn_rate * received_ref[...].astype(f32)).astype(bf16)


def finish(which, base_term, received, start, total_rows, previous):
    block = base_term.shape[0]
    count, width = received.shape
    rows = 128
    in_specs = [
        pl.BlockSpec((rows, width), lambda s, b: (start // rows + s, 0)),
        pl.BlockSpec((rows, width), lambda s, b: (s, 0)),
    ]
    operands = [which, base_term, received]
    aliases = {}
    if previous is not None:
        in_specs.append(ANY)
        aliases = {len(operands): 0}
        operands.append(previous)
    return pl.pallas_call(
        finish_kernel,
        grid_spec=pltpu.PrefetchScalarGridSpec(
            num_scalar_prefetch=1,
            grid=(count // rows,),
            in_specs=in_specs,
            out_specs=pl.BlockSpec(
                (1, rows, width), lambda s, b: (0, (b[0] * block + start) // rows + s, 0)
            ),
        ),
        out_shape=jax.ShapeDtypeStruct((1, total_rows, width), bf16),
        input_output_aliases=aliases,
        cost_estimate=cost(2 * count * width, 8 * count * width),
        compiler_params=limit(8),
    )(*operands)


def on_device(weight, grad, first_moment, second_moment, left_basis, right_basis):
    _, rows, _ = grad.shape
    block = right_basis.shape[1]
    near_block = lax.axis_index("z") // 2
    far_block = 1 - near_block
    near_id = near_block.reshape(1)
    far_id = far_block.reshape(1)

    own_near = lax.dynamic_slice_in_dim(grad, near_block * block, block, axis=1)
    other_near = permute(own_near, "y", near)

    sums = every_sum(jnp.sum(jnp.square(grad.astype(f32))).reshape(1, 1, 1))
    row, left_near, left_far = gather_left(left_basis)

    later_block, _ = lax.optimization_barrier((far_block, row))
    own_far = lax.dynamic_slice_in_dim(grad, later_block * block, block, axis=1)
    other_far = permute(own_far, "y", near)

    term = rotate_right(own_near, other_near, right_basis)
    nf, ns, send, turned = moments(
        True, near_id, sums, left_near, term, right_basis, first_moment, second_moment, None
    )
    received_near = permute(send, "y", near)
    base_near = base(near_id, turned, right_basis, weight)

    term = rotate_right(own_far, other_far, right_basis)
    nf, ns, send, turned = moments(
        False, far_id, sums, left_far, term, right_basis, first_moment, second_moment, (nf, ns)
    )
    received_far = [permute(send[start : start + size], "y", near) for start, size in PIECES]
    base_far = base(far_id, turned, right_basis, weight)

    new_weight = finish(near_id, base_near, received_near, 0, rows, None)
    for i, (start, size) in enumerate(PIECES):
        new_weight = finish(far_id, base_far, received_far[i], start, rows, new_weight)
    return (new_weight, nf, ns)


def solution(mesh):
    finer = Mesh(mesh.devices.reshape(4, 2, 4, 4), AXES)
    spec = P(EXPERT, None, TILE)
    return jax.shard_map(
        on_device, mesh=finer, in_specs=(spec,) * 6, out_specs=(spec,) * 3, check_vma=False
    )
```

```python
import functools

import jax
import jax.numpy as jnp
from jax import lax
from jax.experimental import pallas as pl
from jax.experimental.pallas import tpu as pltpu
from jax.sharding import Mesh
from jax.sharding import PartitionSpec as P


AXES = ("x", "core", "z", "y")
EXPERT = ("x", "core")
TILE = ("z", "y")

beta_one = 0.9
beta_two = 0.95
epsilon = 1e-08
learn_rate = 0.25
decay_rate = 0.1


f32 = jnp.float32
bf16 = jnp.bfloat16
ANY = pl.BlockSpec(memory_space=pl.ANY)
HBM = pl.BlockSpec(memory_space=pltpu.HBM)
MIB = 1024 * 1024
PIECES = ((0, 512), (512, 384), (896, 128))


def cost(flops, bytes_accessed):
    return pl.CostEstimate(flops=flops, bytes_accessed=bytes_accessed, transcendentals=0)


def limit(mib):
    return pltpu.CompilerParams(vmem_limit_bytes=mib * MIB)


def near(i):
    return i ^ 1


def far(i):
    return 3 - i


def permute(value, axis, target):
    pairs = [(source, target(source)) for source in range(lax.axis_size(axis))]
    return lax.ppermute(value, axis, pairs)


def every_sum(value):
    devices = lax.axis_size(AXES)
    return lax.all_to_all(jnp.broadcast_to(value, (devices, 1, 128)), AXES, 0, 0, tiled=True)


def gather_left(shard):
    row = jnp.concatenate((shard, permute(shard, "y", near)), axis=1)
    row_far = permute(row, "y", far)
    near0 = permute(row, "z", near)
    far0 = permute(row, "z", far)
    near1 = permute(row_far, "z", near)
    far1 = permute(row_far, "z", far)
    near2 = permute(far0, "z", near)
    far3 = permute(near1, "z", far)
    return (row, row_far, near0, near1), (far0, far1, near2, far3)


def halves(right, y, width):
    position = lax.rem(y, 2)
    own = right[pl.ds(pl.multiple_of(position * width, width), width), :]
    other = right[pl.ds(pl.multiple_of((1 - position) * width, width), width), :]
    return own, other


def start_all(copies):
    for copy in copies:
        copy.start()


def wait_all(copies):
    for copy in copies:
        copy.wait()


def rotate_right_kernel(own_ref, other_ref, right_ref, out_ref, own, other, right, out, sems):
    block, width = out.shape
    rows = 256
    steps = block // rows
    chunks = [pl.ds(s * rows, rows) for s in range(steps)]
    load = pltpu.make_async_copy(right_ref.at[0], right, sems.at[0])
    loads = [
        (
            pltpu.make_async_copy(own_ref.at[0, c, :], own.at[c, :], sems.at[1 + 3 * s]),
            pltpu.make_async_copy(other_ref.at[0, c, :], other.at[c, :], sems.at[2 + 3 * s]),
        )
        for s, c in enumerate(chunks)
    ]
    stores = [
        pltpu.make_async_copy(out.at[c, :], out_ref.at[c, :], sems.at[3 + 3 * s])
        for s, c in enumerate(chunks)
    ]
    load.start()
    for pair in loads:
        start_all(pair)
    load.wait()
    right_own, right_other = halves(right, lax.axis_index("y"), width)
    for s, c in enumerate(chunks):
        wait_all(loads[s])
        out[c, :] = (
            jnp.dot(own[c, :], right_own, preferred_element_type=f32)
            + jnp.dot(other[c, :], right_other, preferred_element_type=f32)
        ).astype(bf16)
        stores[s].start()
    wait_all(stores)


def rotate_right(own, other, right):
    _, block, width = own.shape
    half = pltpu.VMEM((block, width), bf16)
    return pl.pallas_call(
        rotate_right_kernel,
        out_shape=jax.ShapeDtypeStruct((block, width), bf16),
        in_specs=[HBM] * 3,
        out_specs=HBM,
        scratch_shapes=[half, half, half, half, pltpu.SemaphoreType.DMA((13,))],
        cost_estimate=cost(4 * block * width * width, 8 * block * width),
        compiler_params=limit(63),
    )(own, other, right)


def moments_kernel(is_near, count, pieces, block_ref, sums_ref, *refs):
    shards = refs[:4]
    term_ref, right_ref, first_ref, second_ref = refs[4:8]
    new_first_ref, new_second_ref, turned_ref, *send_refs = refs[-12 - len(pieces) : -9]
    left, term, right, first, second, update, turned, send, sems = refs[-9:]
    block, width = term.shape
    rows = 256
    steps = block // rows
    z = lax.axis_index("z")
    y = lax.axis_index("y")
    base_row = block_ref[0] * block
    chunks = [pl.ds(s * rows, rows) for s in range(steps)]
    places = [pl.ds(pl.multiple_of(base_row + s * rows, rows), rows) for s in range(steps)]
    used = [0]

    def copy(source, target):
        used[0] += 1
        return pltpu.make_async_copy(source, target, sems.at[used[0] - 1])

    partner = y + 1 - 2 * lax.rem(y, 2)
    columns = (y, partner, 3 - y, 3 - partner)
    parity = lax.rem(z if is_near else z + 1, 2)
    entry = []
    for k in range(8):
        group, part = k // 2, k % 2
        row = parity if group < 2 else 1 - parity
        slot = row * 4 + columns[k % 4]
        entry.append(
            copy(
                shards[group].at[0, pl.ds(part * block, block), :],
                left.at[:, pl.ds(pl.multiple_of(slot * 128, 128), 128)],
            )
        )
    entry.append(copy(term_ref, term))
    loads = [
        (copy(first_ref.at[0, p, :], first.at[c, :]), copy(second_ref.at[0, p, :], second.at[c, :]))
        for c, p in zip(chunks, places)
    ]
    load_right = copy(right_ref.at[0], right)
    stores = [
        (
            copy(first.at[c, :], new_first_ref.at[0, p, :]),
            copy(second.at[c, :], new_second_ref.at[0, p, :]),
        )
        for c, p in zip(chunks, places)
    ]
    start_all(entry)
    for pair in loads:
        start_all(pair)
    load_right.start()

    total = jnp.sum(sums_ref[...], axis=0)
    clip = 1.0 / jnp.maximum(1.0, jnp.sqrt(total / count))
    clip = jnp.concatenate([clip] * (width // 128), axis=1)
    wait_all(entry)

    def rotate(s):
        return lax.dot_general(
            left[:, chunks[s]], term[...], (((0,), (0,)), ((), ())), preferred_element_type=f32
        )

    rotated = rotate(0)
    for s, c in enumerate(chunks):
        wait_all(loads[s])
        following = rotate(s + 1) if s + 1 < steps else None
        clipped = clip * rotated
        new_first = beta_one * first[c, :] + (1.0 - beta_one) * clipped
        new_second = beta_two * second[c, :] + (1.0 - beta_two) * clipped * clipped
        first[c, :] = new_first
        second[c, :] = new_second
        update[c, :] = (new_first / (jnp.sqrt(new_second) + epsilon)).astype(bf16)
        if s > 0:
            start_all(stores[s - 1])
        rotated = following

    load_right.wait()
    _, right_other = halves(right, y, width)
    send_stores = []
    for s, c in enumerate(chunks):
        piece = jnp.dot(left[c, :], update[...], preferred_element_type=f32).astype(bf16)
        turned[c, :] = piece
        send[c, :] = lax.dot_general(
            piece, right_other, (((1,), (1,)), ((), ())), preferred_element_type=f32
        ).astype(bf16)
        if s == 0:
            start_all(stores[steps - 1])
        for (start, size), send_ref in zip(pieces, send_refs):
            low, high = max(start, s * rows), min(start + size, (s + 1) * rows)
            if low < high:
                one = copy(
                    send.at[pl.ds(low, high - low), :],
                    send_ref.at[pl.ds(low - start, high - low), :],
                )
                one.start()
                send_stores.append(one)
    store_turned = copy(turned, turned_ref)
    store_turned.start()
    for pair in stores:
        wait_all(pair)
    wait_all(send_stores)
    store_turned.wait()


def moments(is_near, which, sums, shards, term, right, first, second, previous, pieces):
    _, all_rows, width = first.shape
    block = right.shape[1]
    count = sums.shape[0] * all_rows * width
    whole = jax.ShapeDtypeStruct((1, all_rows, width), f32)
    part = jax.ShapeDtypeStruct((block, width), bf16)
    sends = [jax.ShapeDtypeStruct((size, width), bf16) for _, size in pieces]
    operands = [which, sums, *shards, term, right, first, second]
    aliases = {}
    if previous is not None:
        aliases = {len(operands): 0, len(operands) + 1: 1}
        operands += list(previous)
    in_specs = [pl.BlockSpec(memory_space=pltpu.SMEM), pl.BlockSpec(memory_space=pltpu.VMEM)]
    in_specs += [HBM] * (len(operands) - 2)
    half = pltpu.VMEM((block, width), bf16)
    moment = pltpu.VMEM((block, width), f32)
    return pl.pallas_call(
        functools.partial(moments_kernel, is_near, count, pieces),
        out_shape=[whole, whole, part, *sends],
        in_specs=in_specs,
        out_specs=[HBM] * (3 + len(sends)),
        scratch_shapes=[
            pltpu.VMEM((block, block), bf16),
            half,
            half,
            moment,
            moment,
            half,
            half,
            half,
            pltpu.SemaphoreType.DMA((40,)),
        ],
        input_output_aliases=aliases,
        cost_estimate=cost(5 * block * block * width, 20 * block * width),
        compiler_params=limit(63),
    )(*operands)


def base_kernel(block_ref, turned_ref, right_ref, weight_ref, out_ref):
    width = right_ref.shape[2]
    position = lax.rem(lax.axis_index("y"), 2)
    right_own = right_ref[0, pl.ds(pl.multiple_of(position * width, width), width), :]
    back = lax.dot_general(
        turned_ref[...], right_own, (((1,), (1,)), ((), ())), preferred_element_type=f32
    )
    weight = weight_ref[0].astype(f32)
    out_ref[...] = weight - learn_rate * (back + decay_rate * weight)


def base(which, turned, right, weight):
    block, width = turned.shape
    rows = 256
    steps = block // rows
    return pl.pallas_call(
        base_kernel,
        grid_spec=pltpu.PrefetchScalarGridSpec(
            num_scalar_prefetch=1,
            grid=(steps,),
            in_specs=[
                pl.BlockSpec((rows, width), lambda s, b: (s, 0)),
                pl.BlockSpec((1, block, width), lambda s, b: (0, 0, 0)),
                pl.BlockSpec((1, rows, width), lambda s, b: (0, b[0] * steps + s, 0)),
            ],
            out_specs=pl.BlockSpec((rows, width), lambda s, b: (s, 0)),
        ),
        out_shape=jax.ShapeDtypeStruct((block, width), f32),
        cost_estimate=cost(2 * block * width * width, 10 * block * width),
        compiler_params=limit(12),
    )(which, turned, right, weight)


def finish_kernel(block_ref, base_ref, received_ref, *refs):
    refs[-1][0] = (base_ref[...] - learn_rate * received_ref[...].astype(f32)).astype(bf16)


def finish(which, base_term, received, start, total_rows, previous):
    block = base_term.shape[0]
    count, width = received.shape
    rows = 128
    in_specs = [
        pl.BlockSpec((rows, width), lambda s, b: (start // rows + s, 0)),
        pl.BlockSpec((rows, width), lambda s, b: (s, 0)),
    ]
    operands = [which, base_term, received]
    aliases = {}
    if previous is not None:
        in_specs.append(ANY)
        aliases = {len(operands): 0}
        operands.append(previous)
    return pl.pallas_call(
        finish_kernel,
        grid_spec=pltpu.PrefetchScalarGridSpec(
            num_scalar_prefetch=1,
            grid=(count // rows,),
            in_specs=in_specs,
            out_specs=pl.BlockSpec(
                (1, rows, width), lambda s, b: (0, (b[0] * block + start) // rows + s, 0)
            ),
        ),
        out_shape=jax.ShapeDtypeStruct((1, total_rows, width), bf16),
        input_output_aliases=aliases,
        cost_estimate=cost(2 * count * width, 8 * count * width),
        compiler_params=limit(8),
    )(*operands)


def on_device(weight, grad, first_moment, second_moment, left_basis, right_basis):
    _, rows, _ = grad.shape
    block = right_basis.shape[1]
    near_block = lax.axis_index("z") // 2
    far_block = 1 - near_block
    near_id = near_block.reshape(1)
    far_id = far_block.reshape(1)

    own_near = lax.dynamic_slice_in_dim(grad, near_block * block, block, axis=1)
    other_near = permute(own_near, "y", near)

    local_sum = jnp.sum(jnp.square(grad.astype(f32))).reshape(1, 1, 1)
    sums = every_sum(local_sum)
    left_near, left_far = gather_left(left_basis)

    own_far = lax.dynamic_slice_in_dim(grad, far_block * block, block, axis=1)
    other_far = permute(own_far, "y", near)

    term = rotate_right(own_near, other_near, right_basis)
    nf, ns, turned, send = moments(
        True, near_id, sums, left_near, term, right_basis, first_moment, second_moment, None,
        ((0, block),),
    )
    received_near = permute(send, "y", near)
    base_near = base(near_id, turned, right_basis, weight)

    term = rotate_right(own_far, other_far, right_basis)
    nf, ns, turned, *sends = moments(
        False, far_id, sums, left_far, term, right_basis, first_moment, second_moment, (nf, ns),
        PIECES,
    )
    received_far = [permute(send, "y", near) for send in sends]
    base_far = base(far_id, turned, right_basis, weight)

    new_weight = finish(near_id, base_near, received_near, 0, rows, None)
    for i, (start, size) in enumerate(PIECES):
        new_weight = finish(far_id, base_far, received_far[i], start, rows, new_weight)
    return (new_weight, nf, ns)


def solution(mesh):
    finer = Mesh(mesh.devices.reshape(4, 2, 4, 4), AXES)
    spec = P(EXPERT, None, TILE)
    return jax.shard_map(
        on_device, mesh=finer, in_specs=(spec,) * 6, out_specs=(spec,) * 3, check_vma=False
    )
```

```python
import functools

import jax
import jax.numpy as jnp
from jax import lax
from jax.experimental import pallas as pl
from jax.experimental.pallas import tpu as pltpu
from jax.sharding import Mesh
from jax.sharding import PartitionSpec as P


AXES = ("x", "core", "z", "y")
EXPERT = ("x", "core")
TILE = ("z", "y")

beta_one = 0.9
beta_two = 0.95
epsilon = 1e-08
learn_rate = 0.25
decay_rate = 0.1


f32 = jnp.float32
bf16 = jnp.bfloat16
ANY = pl.BlockSpec(memory_space=pl.ANY)
HBM = pl.BlockSpec(memory_space=pltpu.HBM)
MIB = 1024 * 1024
PIECES = ((0, 512), (512, 384), (896, 128))


def cost(flops, bytes_accessed):
    return pl.CostEstimate(flops=flops, bytes_accessed=bytes_accessed, transcendentals=0)


def limit(mib):
    return pltpu.CompilerParams(vmem_limit_bytes=mib * MIB)


def near(i):
    return i ^ 1


def far(i):
    return 3 - i


def permute(value, axis, target):
    pairs = [(source, target(source)) for source in range(lax.axis_size(axis))]
    return lax.ppermute(value, axis, pairs)


def every_sum(value):
    value = value + permute(value, "y", near)
    value = value + permute(value, "y", far)
    axes = ("x", "core", "z")
    return lax.all_to_all(
        jnp.broadcast_to(value, (lax.axis_size(axes), 1, 128)), axes, 0, 0, tiled=True
    )


def split_kernel(block_ref, first_ref, second_ref, near_ref, far_ref, sum_ref, partial):
    step = pl.program_id(0)

    @pl.when(step == 0)
    def _():
        partial[...] = jnp.zeros_like(partial)

    near_ref[...] = first_ref[...]
    far_ref[...] = second_ref[...]
    one = first_ref[0].astype(f32)
    two = second_ref[0].astype(f32)
    squares = (one * one + two * two).reshape(-1, *partial.shape)
    partial[...] += jnp.sum(squares, axis=0)

    @pl.when(step == pl.num_programs(0) - 1)
    def _():
        sum_ref[0] = jnp.broadcast_to(jnp.sum(partial[...], keepdims=True), (1, 128))


def split(which, grad, block):
    _, _, width = grad.shape
    rows = 512
    steps = block // rows
    half = jax.ShapeDtypeStruct((1, block, width), bf16)
    chunk = pl.BlockSpec((1, rows, width), lambda s, b: (0, s, 0))
    return pl.pallas_call(
        split_kernel,
        grid_spec=pltpu.PrefetchScalarGridSpec(
            num_scalar_prefetch=1,
            grid=(steps,),
            in_specs=[
                pl.BlockSpec((1, rows, width), lambda s, b: (0, b[0] * steps + s, 0)),
                pl.BlockSpec((1, rows, width), lambda s, b: (0, (1 - b[0]) * steps + s, 0)),
            ],
            out_specs=[chunk, chunk, pl.BlockSpec((1, 1, 128), lambda s, b: (0, 0, 0))],
            scratch_shapes=[pltpu.VMEM((8, width), f32)],
        ),
        out_shape=[half, half, jax.ShapeDtypeStruct((1, 1, 128), f32)],
        cost_estimate=cost(4 * block * width, 8 * block * width),
        compiler_params=limit(63),
        name="split",
    )(which, grad, grad)


def gather_left(shard):
    row = jnp.concatenate((shard, permute(shard, "y", near)), axis=1)
    row_far = permute(row, "y", far)
    near0 = permute(row, "z", near)
    far0 = permute(row, "z", far)
    near1 = permute(row_far, "z", near)
    far1 = permute(row_far, "z", far)
    near2 = permute(far0, "z", near)
    far3 = permute(near1, "z", far)
    return (row, row_far, near0, near1), (far0, far1, near2, far3)


def halves(right, y, width):
    position = lax.rem(y, 2)
    own = right[pl.ds(pl.multiple_of(position * width, width), width), :]
    other = right[pl.ds(pl.multiple_of((1 - position) * width, width), width), :]
    return own, other


def start_all(copies):
    for copy in copies:
        copy.start()


def wait_all(copies):
    for copy in copies:
        copy.wait()


def rotate_right_kernel(own_ref, other_ref, right_ref, out_ref, own, other, right, out, sems):
    block, width = out.shape
    rows = 256
    steps = block // rows
    chunks = [pl.ds(s * rows, rows) for s in range(steps)]
    load = pltpu.make_async_copy(right_ref.at[0], right, sems.at[0])
    loads = [
        (
            pltpu.make_async_copy(own_ref.at[0, c, :], own.at[c, :], sems.at[1 + 3 * s]),
            pltpu.make_async_copy(other_ref.at[0, c, :], other.at[c, :], sems.at[2 + 3 * s]),
        )
        for s, c in enumerate(chunks)
    ]
    stores = [
        pltpu.make_async_copy(out.at[c, :], out_ref.at[c, :], sems.at[3 + 3 * s])
        for s, c in enumerate(chunks)
    ]
    load.start()
    for pair in loads:
        start_all(pair)
    load.wait()
    right_own, right_other = halves(right, lax.axis_index("y"), width)
    for s, c in enumerate(chunks):
        wait_all(loads[s])
        out[c, :] = (
            jnp.dot(own[c, :], right_own, preferred_element_type=f32)
            + jnp.dot(other[c, :], right_other, preferred_element_type=f32)
        ).astype(bf16)
        stores[s].start()
    wait_all(stores)


def rotate_right(own, other, right):
    _, block, width = own.shape
    half = pltpu.VMEM((block, width), bf16)
    return pl.pallas_call(
        rotate_right_kernel,
        out_shape=jax.ShapeDtypeStruct((block, width), bf16),
        in_specs=[HBM] * 3,
        out_specs=HBM,
        scratch_shapes=[half, half, half, half, pltpu.SemaphoreType.DMA((13,))],
        cost_estimate=cost(4 * block * width * width, 8 * block * width),
        compiler_params=limit(63),
    )(own, other, right)


def moments_kernel(is_near, count, pieces, block_ref, sums_ref, *refs):
    shards = refs[:4]
    term_ref, right_ref, first_ref, second_ref = refs[4:8]
    new_first_ref, new_second_ref, turned_ref, *send_refs = refs[-12 - len(pieces) : -9]
    left, term, right, first, second, update, turned, send, sems = refs[-9:]
    block, width = term.shape
    rows = 256
    steps = block // rows
    z = lax.axis_index("z")
    y = lax.axis_index("y")
    base_row = block_ref[0] * block
    chunks = [pl.ds(s * rows, rows) for s in range(steps)]
    places = [pl.ds(pl.multiple_of(base_row + s * rows, rows), rows) for s in range(steps)]
    used = [0]

    def copy(source, target):
        used[0] += 1
        return pltpu.make_async_copy(source, target, sems.at[used[0] - 1])

    partner = y + 1 - 2 * lax.rem(y, 2)
    columns = (y, partner, 3 - y, 3 - partner)
    parity = lax.rem(z if is_near else z + 1, 2)
    entry = []
    for k in range(8):
        group, part = k // 2, k % 2
        row = parity if group < 2 else 1 - parity
        slot = row * 4 + columns[k % 4]
        entry.append(
            copy(
                shards[group].at[0, pl.ds(part * block, block), :],
                left.at[:, pl.ds(pl.multiple_of(slot * 128, 128), 128)],
            )
        )
    entry.append(copy(term_ref, term))
    loads = [
        (copy(first_ref.at[0, p, :], first.at[c, :]), copy(second_ref.at[0, p, :], second.at[c, :]))
        for c, p in zip(chunks, places)
    ]
    load_right = copy(right_ref.at[0], right)
    stores = [
        (
            copy(first.at[c, :], new_first_ref.at[0, p, :]),
            copy(second.at[c, :], new_second_ref.at[0, p, :]),
        )
        for c, p in zip(chunks, places)
    ]
    start_all(entry)
    for pair in loads:
        start_all(pair)
    load_right.start()

    total = jnp.sum(sums_ref[...], axis=0)
    clip = 1.0 / jnp.maximum(1.0, jnp.sqrt(total / count))
    clip = jnp.concatenate([clip] * (width // 128), axis=1)
    wait_all(entry)

    def rotate(s):
        return lax.dot_general(
            left[:, chunks[s]], term[...], (((0,), (0,)), ((), ())), preferred_element_type=f32
        )

    rotated = rotate(0)
    for s, c in enumerate(chunks):
        wait_all(loads[s])
        following = rotate(s + 1) if s + 1 < steps else None
        clipped = clip * rotated
        new_first = beta_one * first[c, :] + (1.0 - beta_one) * clipped
        new_second = beta_two * second[c, :] + (1.0 - beta_two) * clipped * clipped
        first[c, :] = new_first
        second[c, :] = new_second
        update[c, :] = (new_first / (jnp.sqrt(new_second) + epsilon)).astype(bf16)
        if s > 0:
            start_all(stores[s - 1])
        rotated = following

    load_right.wait()
    _, right_other = halves(right, y, width)
    send_stores = []
    for s, c in enumerate(chunks):
        piece = jnp.dot(left[c, :], update[...], preferred_element_type=f32).astype(bf16)
        turned[c, :] = piece
        send[c, :] = lax.dot_general(
            piece, right_other, (((1,), (1,)), ((), ())), preferred_element_type=f32
        ).astype(bf16)
        if s == 0:
            start_all(stores[steps - 1])
        for (start, size), send_ref in zip(pieces, send_refs):
            low, high = max(start, s * rows), min(start + size, (s + 1) * rows)
            if low < high:
                one = copy(
                    send.at[pl.ds(low, high - low), :],
                    send_ref.at[pl.ds(low - start, high - low), :],
                )
                one.start()
                send_stores.append(one)
    store_turned = copy(turned, turned_ref)
    store_turned.start()
    for pair in stores:
        wait_all(pair)
    wait_all(send_stores)
    store_turned.wait()


def moments(is_near, which, sums, shards, term, right, first, second, previous, pieces):
    _, all_rows, width = first.shape
    block = right.shape[1]
    count = lax.axis_size(AXES) * all_rows * width
    whole = jax.ShapeDtypeStruct((1, all_rows, width), f32)
    part = jax.ShapeDtypeStruct((block, width), bf16)
    sends = [jax.ShapeDtypeStruct((size, width), bf16) for _, size in pieces]
    operands = [which, sums, *shards, term, right, first, second]
    aliases = {}
    if previous is not None:
        aliases = {len(operands): 0, len(operands) + 1: 1}
        operands += list(previous)
    in_specs = [pl.BlockSpec(memory_space=pltpu.SMEM), pl.BlockSpec(memory_space=pltpu.VMEM)]
    in_specs += [HBM] * (len(operands) - 2)
    half = pltpu.VMEM((block, width), bf16)
    moment = pltpu.VMEM((block, width), f32)
    return pl.pallas_call(
        functools.partial(moments_kernel, is_near, count, pieces),
        out_shape=[whole, whole, part, *sends],
        in_specs=in_specs,
        out_specs=[HBM] * (3 + len(sends)),
        scratch_shapes=[
            pltpu.VMEM((block, block), bf16),
            half,
            half,
            moment,
            moment,
            half,
            half,
            half,
            pltpu.SemaphoreType.DMA((40,)),
        ],
        input_output_aliases=aliases,
        cost_estimate=cost(5 * block * block * width, 20 * block * width),
        compiler_params=limit(63),
    )(*operands)


def base_kernel(block_ref, turned_ref, right_ref, weight_ref, out_ref):
    width = right_ref.shape[2]
    position = lax.rem(lax.axis_index("y"), 2)
    right_own = right_ref[0, pl.ds(pl.multiple_of(position * width, width), width), :]
    back = lax.dot_general(
        turned_ref[...], right_own, (((1,), (1,)), ((), ())), preferred_element_type=f32
    )
    weight = weight_ref[0].astype(f32)
    out_ref[...] = weight - learn_rate * (back + decay_rate * weight)


def base(which, turned, right, weight):
    block, width = turned.shape
    rows = 256
    steps = block // rows
    return pl.pallas_call(
        base_kernel,
        grid_spec=pltpu.PrefetchScalarGridSpec(
            num_scalar_prefetch=1,
            grid=(steps,),
            in_specs=[
                pl.BlockSpec((rows, width), lambda s, b: (s, 0)),
                pl.BlockSpec((1, block, width), lambda s, b: (0, 0, 0)),
                pl.BlockSpec((1, rows, width), lambda s, b: (0, b[0] * steps + s, 0)),
            ],
            out_specs=pl.BlockSpec((rows, width), lambda s, b: (s, 0)),
        ),
        out_shape=jax.ShapeDtypeStruct((block, width), f32),
        cost_estimate=cost(2 * block * width * width, 10 * block * width),
        compiler_params=limit(12),
    )(which, turned, right, weight)


def finish_kernel(block_ref, base_ref, received_ref, *refs):
    refs[-1][0] = (base_ref[...] - learn_rate * received_ref[...].astype(f32)).astype(bf16)


def finish(which, base_term, received, start, total_rows, previous):
    block = base_term.shape[0]
    count, width = received.shape
    rows = 128
    in_specs = [
        pl.BlockSpec((rows, width), lambda s, b: (start // rows + s, 0)),
        pl.BlockSpec((rows, width), lambda s, b: (s, 0)),
    ]
    operands = [which, base_term, received]
    aliases = {}
    if previous is not None:
        in_specs.append(ANY)
        aliases = {len(operands): 0}
        operands.append(previous)
    return pl.pallas_call(
        finish_kernel,
        grid_spec=pltpu.PrefetchScalarGridSpec(
            num_scalar_prefetch=1,
            grid=(count // rows,),
            in_specs=in_specs,
            out_specs=pl.BlockSpec(
                (1, rows, width), lambda s, b: (0, (b[0] * block + start) // rows + s, 0)
            ),
        ),
        out_shape=jax.ShapeDtypeStruct((1, total_rows, width), bf16),
        input_output_aliases=aliases,
        cost_estimate=cost(2 * count * width, 8 * count * width),
        compiler_params=limit(8),
    )(*operands)


def on_device(weight, grad, first_moment, second_moment, left_basis, right_basis):
    _, rows, _ = grad.shape
    block = right_basis.shape[1]
    near_block = lax.axis_index("z") // 2
    far_block = 1 - near_block
    near_id = near_block.reshape(1)
    far_id = far_block.reshape(1)

    own_near, own_far, local_sum = split(near_id, grad, block)
    other_near = permute(own_near, "y", near)
    sums = every_sum(local_sum)
    left_near, left_far = gather_left(left_basis)

    other_far = permute(own_far, "y", near)

    term = rotate_right(own_near, other_near, right_basis)
    nf, ns, turned, send = moments(
        True, near_id, sums, left_near, term, right_basis, first_moment, second_moment, None,
        ((0, block),),
    )
    received_near = permute(send, "y", near)
    base_near = base(near_id, turned, right_basis, weight)

    term = rotate_right(own_far, other_far, right_basis)
    nf, ns, turned, *sends = moments(
        False, far_id, sums, left_far, term, right_basis, first_moment, second_moment, (nf, ns),
        PIECES,
    )
    received_far = [permute(send, "y", near) for send in sends]
    base_far = base(far_id, turned, right_basis, weight)

    new_weight = finish(near_id, base_near, received_near, 0, rows, None)
    for i, (start, size) in enumerate(PIECES):
        new_weight = finish(far_id, base_far, received_far[i], start, rows, new_weight)
    return (new_weight, nf, ns)


def solution(mesh):
    finer = Mesh(mesh.devices.reshape(4, 2, 4, 4), AXES)
    spec = P(EXPERT, None, TILE)
    return jax.shard_map(
        on_device, mesh=finer, in_specs=(spec,) * 6, out_specs=(spec,) * 3, check_vma=False
    )
```

```python
import functools

import jax
import jax.numpy as jnp
from jax import lax
from jax.experimental import pallas as pl
from jax.experimental.pallas import tpu as pltpu
from jax.sharding import Mesh
from jax.sharding import PartitionSpec as P


AXES = ("x", "core", "z", "y")
EXPERT = ("x", "core")
TILE = ("z", "y")

beta_one = 0.9
beta_two = 0.95
epsilon = 1e-08
learn_rate = 0.25
decay_rate = 0.1


f32 = jnp.float32
bf16 = jnp.bfloat16
ANY = pl.BlockSpec(memory_space=pl.ANY)
HBM = pl.BlockSpec(memory_space=pltpu.HBM)
MIB = 1024 * 1024
PIECES = ((0, 768), (768, 128), (896, 128))


def cost(flops, bytes_accessed):
    return pl.CostEstimate(flops=flops, bytes_accessed=bytes_accessed, transcendentals=0)


def limit(mib):
    return pltpu.CompilerParams(vmem_limit_bytes=mib * MIB)


def near(i):
    return i ^ 1


def far(i):
    return 3 - i


def permute(value, axis, target):
    pairs = [(source, target(source)) for source in range(lax.axis_size(axis))]
    return lax.ppermute(value, axis, pairs)


def every_sum(value):
    value = value + permute(value, "y", near)
    value = value + permute(value, "y", far)
    axes = ("x", "core", "z")
    return lax.all_to_all(
        jnp.broadcast_to(value, (lax.axis_size(axes), 1, 128)), axes, 0, 0, tiled=True
    )


def split_kernel(block_ref, first_ref, second_ref, near_ref, far_ref, sum_ref, partial):
    step = pl.program_id(0)

    @pl.when(step == 0)
    def _():
        partial[...] = jnp.zeros_like(partial)

    near_ref[...] = first_ref[...]
    far_ref[...] = second_ref[...]
    one = first_ref[0].astype(f32)
    two = second_ref[0].astype(f32)
    squares = (one * one + two * two).reshape(-1, *partial.shape)
    partial[...] += jnp.sum(squares, axis=0)

    @pl.when(step == pl.num_programs(0) - 1)
    def _():
        sum_ref[0] = jnp.broadcast_to(jnp.sum(partial[...], keepdims=True), (1, 128))


def split(which, grad, block):
    _, _, width = grad.shape
    rows = block
    steps = block // rows
    half = jax.ShapeDtypeStruct((1, block, width), bf16)
    chunk = pl.BlockSpec((1, rows, width), lambda s, b: (0, s, 0))
    return pl.pallas_call(
        split_kernel,
        grid_spec=pltpu.PrefetchScalarGridSpec(
            num_scalar_prefetch=1,
            grid=(steps,),
            in_specs=[
                pl.BlockSpec((1, rows, width), lambda s, b: (0, b[0] * steps + s, 0)),
                pl.BlockSpec((1, rows, width), lambda s, b: (0, (1 - b[0]) * steps + s, 0)),
            ],
            out_specs=[chunk, chunk, pl.BlockSpec((1, 1, 128), lambda s, b: (0, 0, 0))],
            scratch_shapes=[pltpu.VMEM((8, width), f32)],
        ),
        out_shape=[half, half, jax.ShapeDtypeStruct((1, 1, 128), f32)],
        cost_estimate=cost(4 * block * width, 8 * block * width),
        compiler_params=limit(63),
        name="split",
    )(which, grad, grad)


def gather_left(shard):
    row = jnp.concatenate((shard, permute(shard, "y", near)), axis=1)
    row_far = permute(row, "y", far)
    near0 = permute(row, "z", near)
    far0 = permute(row, "z", far)
    near1 = permute(row_far, "z", near)
    far1 = permute(row_far, "z", far)
    near2 = permute(far0, "z", near)
    far3 = permute(near1, "z", far)
    return (row, row_far, near0, near1), (far0, far1, near2, far3)


def halves(right, y, width):
    position = lax.rem(y, 2)
    own = right[pl.ds(pl.multiple_of(position * width, width), width), :]
    other = right[pl.ds(pl.multiple_of((1 - position) * width, width), width), :]
    return own, other


def start_all(copies):
    for copy in copies:
        copy.start()


def wait_all(copies):
    for copy in copies:
        copy.wait()


def rotate_right_kernel(own_ref, other_ref, right_ref, out_ref, own, other, right, out, sems):
    block, width = out.shape
    rows = 256
    steps = block // rows
    chunks = [pl.ds(s * rows, rows) for s in range(steps)]
    load = pltpu.make_async_copy(right_ref.at[0], right, sems.at[0])
    loads = [
        (
            pltpu.make_async_copy(own_ref.at[0, c, :], own.at[c, :], sems.at[1 + 3 * s]),
            pltpu.make_async_copy(other_ref.at[0, c, :], other.at[c, :], sems.at[2 + 3 * s]),
        )
        for s, c in enumerate(chunks)
    ]
    stores = [
        pltpu.make_async_copy(out.at[c, :], out_ref.at[c, :], sems.at[3 + 3 * s])
        for s, c in enumerate(chunks)
    ]
    load.start()
    for pair in loads:
        start_all(pair)
    load.wait()
    right_own, right_other = halves(right, lax.axis_index("y"), width)
    for s, c in enumerate(chunks):
        wait_all(loads[s])
        out[c, :] = (
            jnp.dot(own[c, :], right_own, preferred_element_type=f32)
            + jnp.dot(other[c, :], right_other, preferred_element_type=f32)
        ).astype(bf16)
        stores[s].start()
    wait_all(stores)


def rotate_right(own, other, right):
    _, block, width = own.shape
    half = pltpu.VMEM((block, width), bf16)
    return pl.pallas_call(
        rotate_right_kernel,
        out_shape=jax.ShapeDtypeStruct((block, width), bf16),
        in_specs=[HBM] * 3,
        out_specs=HBM,
        scratch_shapes=[half, half, half, half, pltpu.SemaphoreType.DMA((13,))],
        cost_estimate=cost(4 * block * width * width, 8 * block * width),
        compiler_params=limit(63),
    )(own, other, right)


def moments_kernel(is_near, count, pieces, block_ref, sums_ref, *refs):
    shards = refs[:4]
    term_ref, right_ref, first_ref, second_ref = refs[4:8]
    new_first_ref, new_second_ref, turned_ref, *send_refs = refs[-12 - len(pieces) : -9]
    left, term, right, first, second, update, turned, send, sems = refs[-9:]
    block, width = term.shape
    rows = 256
    steps = block // rows
    z = lax.axis_index("z")
    y = lax.axis_index("y")
    base_row = block_ref[0] * block
    chunks = [pl.ds(s * rows, rows) for s in range(steps)]
    places = [pl.ds(pl.multiple_of(base_row + s * rows, rows), rows) for s in range(steps)]
    used = [0]

    def copy(source, target):
        used[0] += 1
        return pltpu.make_async_copy(source, target, sems.at[used[0] - 1])

    partner = y + 1 - 2 * lax.rem(y, 2)
    columns = (y, partner, 3 - y, 3 - partner)
    parity = lax.rem(z if is_near else z + 1, 2)
    entry = []
    for k in range(8):
        group, part = k // 2, k % 2
        row = parity if group < 2 else 1 - parity
        slot = row * 4 + columns[k % 4]
        entry.append(
            copy(
                shards[group].at[0, pl.ds(part * block, block), :],
                left.at[:, pl.ds(pl.multiple_of(slot * 128, 128), 128)],
            )
        )
    entry.append(copy(term_ref, term))
    loads = [
        (copy(first_ref.at[0, p, :], first.at[c, :]), copy(second_ref.at[0, p, :], second.at[c, :]))
        for c, p in zip(chunks, places)
    ]
    load_right = copy(right_ref.at[0], right)
    stores = [
        (
            copy(first.at[c, :], new_first_ref.at[0, p, :]),
            copy(second.at[c, :], new_second_ref.at[0, p, :]),
        )
        for c, p in zip(chunks, places)
    ]
    start_all(entry)
    for pair in loads:
        start_all(pair)
    load_right.start()

    total = jnp.sum(sums_ref[...], axis=0)
    clip = 1.0 / jnp.maximum(1.0, jnp.sqrt(total / count))
    clip = jnp.concatenate([clip] * (width // 128), axis=1)
    wait_all(entry)

    def rotate(s):
        return lax.dot_general(
            left[:, chunks[s]], term[...], (((0,), (0,)), ((), ())), preferred_element_type=f32
        )

    rotated = rotate(0)
    for s, c in enumerate(chunks):
        wait_all(loads[s])
        following = rotate(s + 1) if s + 1 < steps else None
        clipped = clip * rotated
        new_first = beta_one * first[c, :] + (1.0 - beta_one) * clipped
        new_second = beta_two * second[c, :] + (1.0 - beta_two) * clipped * clipped
        first[c, :] = new_first
        second[c, :] = new_second
        update[c, :] = (new_first / (jnp.sqrt(new_second) + epsilon)).astype(bf16)
        if s > 0:
            start_all(stores[s - 1])
        rotated = following

    load_right.wait()
    _, right_other = halves(right, y, width)
    send_stores = []
    for s, c in enumerate(chunks):
        piece = jnp.dot(left[c, :], update[...], preferred_element_type=f32).astype(bf16)
        turned[c, :] = piece
        send[c, :] = lax.dot_general(
            piece, right_other, (((1,), (1,)), ((), ())), preferred_element_type=f32
        ).astype(bf16)
        if s == 0:
            start_all(stores[steps - 1])
        for (start, size), send_ref in zip(pieces, send_refs):
            low, high = max(start, s * rows), min(start + size, (s + 1) * rows)
            if low < high:
                one = copy(
                    send.at[pl.ds(low, high - low), :],
                    send_ref.at[pl.ds(low - start, high - low), :],
                )
                one.start()
                send_stores.append(one)
    store_turned = copy(turned, turned_ref)
    store_turned.start()
    for pair in stores:
        wait_all(pair)
    wait_all(send_stores)
    store_turned.wait()


def moments(is_near, which, sums, shards, term, right, first, second, previous, pieces):
    _, all_rows, width = first.shape
    block = right.shape[1]
    count = lax.axis_size(AXES) * all_rows * width
    whole = jax.ShapeDtypeStruct((1, all_rows, width), f32)
    part = jax.ShapeDtypeStruct((block, width), bf16)
    sends = [jax.ShapeDtypeStruct((size, width), bf16) for _, size in pieces]
    operands = [which, sums, *shards, term, right, first, second]
    aliases = {}
    if previous is not None:
        aliases = {len(operands): 0, len(operands) + 1: 1}
        operands += list(previous)
    in_specs = [pl.BlockSpec(memory_space=pltpu.SMEM), pl.BlockSpec(memory_space=pltpu.VMEM)]
    in_specs += [HBM] * (len(operands) - 2)
    half = pltpu.VMEM((block, width), bf16)
    moment = pltpu.VMEM((block, width), f32)
    return pl.pallas_call(
        functools.partial(moments_kernel, is_near, count, pieces),
        out_shape=[whole, whole, part, *sends],
        in_specs=in_specs,
        out_specs=[HBM] * (3 + len(sends)),
        scratch_shapes=[
            pltpu.VMEM((block, block), bf16),
            half,
            half,
            moment,
            moment,
            half,
            half,
            half,
            pltpu.SemaphoreType.DMA((40,)),
        ],
        input_output_aliases=aliases,
        cost_estimate=cost(5 * block * block * width, 20 * block * width),
        compiler_params=limit(63),
    )(*operands)


def base_kernel(block_ref, turned_ref, right_ref, weight_ref, out_ref):
    width = right_ref.shape[2]
    position = lax.rem(lax.axis_index("y"), 2)
    right_own = right_ref[0, pl.ds(pl.multiple_of(position * width, width), width), :]
    back = lax.dot_general(
        turned_ref[...], right_own, (((1,), (1,)), ((), ())), preferred_element_type=f32
    )
    weight = weight_ref[0].astype(f32)
    out_ref[...] = weight - learn_rate * (back + decay_rate * weight)


def base(which, turned, right, weight):
    block, width = turned.shape
    rows = 256
    steps = block // rows
    return pl.pallas_call(
        base_kernel,
        grid_spec=pltpu.PrefetchScalarGridSpec(
            num_scalar_prefetch=1,
            grid=(steps,),
            in_specs=[
                pl.BlockSpec((rows, width), lambda s, b: (s, 0)),
                pl.BlockSpec((1, block, width), lambda s, b: (0, 0, 0)),
                pl.BlockSpec((1, rows, width), lambda s, b: (0, b[0] * steps + s, 0)),
            ],
            out_specs=pl.BlockSpec((rows, width), lambda s, b: (s, 0)),
        ),
        out_shape=jax.ShapeDtypeStruct((block, width), f32),
        cost_estimate=cost(2 * block * width * width, 10 * block * width),
        compiler_params=limit(12),
    )(which, turned, right, weight)


def finish_kernel(block_ref, base_ref, received_ref, *refs):
    refs[-1][0] = (base_ref[...] - learn_rate * received_ref[...].astype(f32)).astype(bf16)


def finish(which, base_term, received, start, total_rows, previous):
    block = base_term.shape[0]
    count, width = received.shape
    rows = 256 if count % 256 == 0 else 128
    in_specs = [
        pl.BlockSpec((rows, width), lambda s, b: (start // rows + s, 0)),
        pl.BlockSpec((rows, width), lambda s, b: (s, 0)),
    ]
    operands = [which, base_term, received]
    aliases = {}
    if previous is not None:
        in_specs.append(ANY)
        aliases = {len(operands): 0}
        operands.append(previous)
    return pl.pallas_call(
        finish_kernel,
        grid_spec=pltpu.PrefetchScalarGridSpec(
            num_scalar_prefetch=1,
            grid=(count // rows,),
            in_specs=in_specs,
            out_specs=pl.BlockSpec(
                (1, rows, width), lambda s, b: (0, (b[0] * block + start) // rows + s, 0)
            ),
        ),
        out_shape=jax.ShapeDtypeStruct((1, total_rows, width), bf16),
        input_output_aliases=aliases,
        cost_estimate=cost(2 * count * width, 8 * count * width),
        compiler_params=limit(8),
    )(*operands)


def on_device(weight, grad, first_moment, second_moment, left_basis, right_basis):
    _, rows, _ = grad.shape
    block = right_basis.shape[1]
    near_block = lax.axis_index("z") // 2
    far_block = 1 - near_block
    near_id = near_block.reshape(1)
    far_id = far_block.reshape(1)

    own_near, own_far, local_sum = split(near_id, grad, block)
    other_near = permute(own_near, "y", near)
    sums = every_sum(local_sum)
    left_near, left_far = gather_left(left_basis)

    other_far = permute(own_far, "y", near)

    term = rotate_right(own_near, other_near, right_basis)
    nf, ns, turned, send = moments(
        True, near_id, sums, left_near, term, right_basis, first_moment, second_moment, None,
        ((0, block),),
    )
    received_near = permute(send, "y", near)
    base_near = base(near_id, turned, right_basis, weight)

    term = rotate_right(own_far, other_far, right_basis)
    nf, ns, turned, *sends = moments(
        False, far_id, sums, left_far, term, right_basis, first_moment, second_moment, (nf, ns),
        PIECES,
    )
    received_far = [permute(send, "y", near) for send in sends]
    base_far = base(far_id, turned, right_basis, weight)

    new_weight = finish(near_id, base_near, received_near, 0, rows, None)
    for i, (start, size) in enumerate(PIECES):
        new_weight = finish(far_id, base_far, received_far[i], start, rows, new_weight)
    return (new_weight, nf, ns)


def solution(mesh):
    finer = Mesh(mesh.devices.reshape(4, 2, 4, 4), AXES)
    spec = P(EXPERT, None, TILE)
    return jax.shard_map(
        on_device, mesh=finer, in_specs=(spec,) * 6, out_specs=(spec,) * 3, check_vma=False
    )
```
